32 devices in a mesh: dp: 8 (over z, x), expert: 4 (over y, core).
Axes of the slice: x: 2, y: 2, z: 4, core: 2. Of those that a mesh axis runs over, the one named last changes fastest.
Arguments:
- tokens: bfloat16 [1024, 4096], P('expert', 'dp'), may hold values from -6 to 6
- cotangent: bfloat16 [1024, 4096], P('expert', 'dp'), may hold values from -6 to 6
- expert_ids: int32 [1024, 2], P('expert'), may hold values from 0 to 3, all different within a row; in each aligned block of 256 rows (0 to 255, 256 to 511, ...) at most 129 rows name the same one
- combine: float32 [1024, 2], P('expert'), may hold values from 0.1 to 1
- w_gate: bfloat16 [4, 4096, 14336], P('expert', None, 'dp'), may hold values from -0.09375 to 0.09375
- w_up: bfloat16 [4, 4096, 14336], P('expert', None, 'dp'), may hold values from -0.09375 to 0.09375
- w_down: bfloat16 [4, 14336, 4096], P('expert', 'dp'), may hold values from -0.046875 to 0.046875
- scale_vector: float32 [4, 14336], P('expert', 'dp'), may hold values from 0.25 to 1.75
Outputs:
- token_grads: bfloat16 [1024, 4096], P('expert', 'dp')
- scale_grads: float32 [4, 14336], P('expert', 'dp')
The draws below stay inside these ranges and needn't reach their ends.
Inputs may be any that keep to these rules, and one draw needn't show every extreme that they name: `expert_ids`: each row names 2 different experts. Among the 256 rows of one aligned block no expert is named more than 129 times, and some block names some expert exactly 129 times.
All inputs are finite; a program needn't handle non-finite values.
Results may differ from the reference program's by a relative error of at most 0.0065.
Values may be sent and summed in bfloat16 or wider, within the bound.
A program may use at most 128 MiB of HBM per device.

```python
import math
import jax
import jax.numpy as jnp
import numpy as np
from jax import lax

D = 4096
FF = 14336
TOP = 2
TOK_DEV = 256
EXPERTS = 4
CAP = 129
TOKENS = 1024


def block_levels(rng, dims, cuts, low, high):
    def one(position, parts):
        heights = jax.random.uniform(jax.random.fold_in(jax.random.fold_in(rng, 6), position), (parts,), jnp.float32, low / len(cuts), high / len(cuts))
        return jnp.repeat(jnp.exp(heights), dims[position] // parts).reshape((-1,) + (1,) * (len(dims) - position - 1))

    loudness = one(*cuts[0])
    for cut in cuts[1:]:
        loudness = loudness * one(*cut)
    return loudness


def routed_block(rng, own, number, rows, number_of, top, most, skew):
    order = jax.random.permutation(rng, number_of)
    crowded, common = load_shares(number_of, rows * top, most, skew, True), load_shares(number_of, rows * top, most, skew, False)
    places = jnp.arange(number_of)

    def named(sizes, offset_by):
        used = int((sizes > 0).sum())
        fixed = max(1, used // 4)
        moved = fixed + (places - fixed + offset_by * (used - fixed)) % max(1, number_of - fixed)
        return jnp.zeros((number_of,), jnp.int32).at[order[jnp.where(places < fixed, places, moved)]].set(jnp.asarray(sizes, jnp.int32))

    sizes = jnp.where(number % 4 == 0, named(crowded, number // 4), named(common, number - number // 4 - 1))
    mixed = jax.random.permutation(jax.random.fold_in(own, 3), number_of)
    giver, sink = mixed[0:number_of // 2 * 2:2], mixed[1:number_of // 2 * 2:2]
    margin = jnp.minimum(sizes[giver] - 1, most - sizes[sink]) // 2
    margin = jnp.where((giver == order[0]) | (sink == order[0]) | (sizes[sink] == 0), 0, jnp.maximum(margin, 0))
    moved = jax.random.randint(jax.random.fold_in(own, 4), (number_of // 2,), 0, 1 << 20) % (margin + 1)
    sizes = sizes.at[giver].add(-moved).at[sink].add(moved)
    items = jnp.searchsorted(jnp.cumsum(sizes), jnp.arange(rows * top), side="right").astype(jnp.int32)
    listing = items.reshape(top, rows).T
    listing = listing[jax.random.permutation(jax.random.fold_in(own, 1), rows)]
    offset_by = jax.random.randint(jax.random.fold_in(own, 2), (rows, 1), 0, top)
    return jnp.take_along_axis(listing, (jnp.arange(top)[None, :] + offset_by) % top, axis=1)


def load_shares(number_of, total, limit, skew, full):
    weights = [(1 << 20) // math.isqrt(grade ** skew) + 1 for grade in range(1, number_of + 1)]
    largest = limit if full else min(limit, max(-(-total // number_of), total * weights[0] // sum(weights)))
    least = 1 if total - largest >= number_of - 1 else 0
    holding, surplus = [largest] + [least] * (number_of - 1), total - largest - least * (number_of - 1)
    while surplus > 0:
        free = [i for i in range(1, number_of) if holding[i] < largest] or [i for i in range(1, number_of) if holding[i] < limit]
        pool, left = sum([weights[i] for i in free]), surplus
        for i in free:
            extra = min(limit - holding[i], max(1, left * weights[i] // pool), surplus)
            holding[i] = holding[i] + extra
            surplus = surplus - extra
    return np.array(holding)


def gaussian(key, shape, deviation, bound, split=(), kind=jnp.bfloat16):
    result = jax.random.normal(key, shape, jnp.float32) * deviation
    if len(split) > 0:
        result = block_levels(key, shape, split, -0.22, 0.18) * result
    return jnp.clip(result, min=-bound, max=bound).astype(kind)


def setup_inputs(seed: int = 0) -> dict:
    streams_of = jax.random.split(jax.random.key(seed), 9)
    tokens = gaussian(streams_of[0], (TOKENS, D), 1.0, 6.0, ((0, 4), (1, 8)))
    cotangent = gaussian(streams_of[1], (TOKENS, D), 1.0, 6.0, ((0, 4), (1, 8)))
    expert_ids_keys = jax.random.split(jax.random.fold_in(streams_of[2], 1), TOKENS // TOK_DEV)
    expert_ids_turns = jax.random.permutation(jax.random.fold_in(streams_of[2], 3), TOKENS // TOK_DEV)
    expert_ids = jax.vmap(lambda own, number: routed_block(jax.random.fold_in(streams_of[2], 2), own, number, TOK_DEV, EXPERTS, TOP, CAP, 2))(expert_ids_keys, expert_ids_turns).reshape((TOKENS, TOP))
    combine = jnp.clip(0.1 + 0.9 * jax.random.uniform(streams_of[3], (TOKENS, TOP), jnp.float32) ** block_levels(streams_of[3], (TOKENS, TOP), ((0, 4),), -0.2, 0.2), 0.1, 1.0)
    w_gate = gaussian(streams_of[4], (EXPERTS, D, FF), D ** -0.5, 0.09375, ((0, 4), (2, 8)))
    w_up = gaussian(streams_of[5], (EXPERTS, D, FF), D ** -0.5, 0.09375, ((0, 4), (2, 8)))
    w_down = gaussian(streams_of[6], (EXPERTS, FF, D), FF ** -0.5, 0.046875, ((0, 4), (1, 8)))
    scale_vector = jnp.clip(1.0 + 0.15 * jax.random.normal(streams_of[7], (EXPERTS, FF), jnp.float32), 0.25, 1.75)
    return dict(tokens=tokens, cotangent=cotangent, expert_ids=expert_ids, combine=combine, w_gate=w_gate, w_up=w_up, w_down=w_down, scale_vector=scale_vector)


def route_tables(expert_ids, combine, experts, capacity):
    blocks = expert_ids.shape[0]
    per_block = expert_ids.shape[1]
    onehot = (expert_ids[:, :, :, None] == jnp.arange(experts, dtype=jnp.int32)).astype(jnp.int32)
    flat_hits = onehot.reshape(blocks, per_block * 2, experts)
    earlier = jnp.cumsum(flat_hits, axis=1) - flat_hits
    slot_ids = jnp.sum(earlier * flat_hits, axis=2).reshape(blocks, per_block, 2)
    positions = (slot_ids[:, :, :, None] == jnp.arange(capacity, dtype=jnp.int32)).astype(jnp.float32)
    matches = onehot.astype(jnp.float32)[:, :, :, :, None] * positions[:, :, :, None, :]
    dispatch = jnp.transpose(jnp.sum(matches, axis=2), (0, 2, 3, 1))
    slot_weight = jnp.sum(matches * combine[:, :, :, None, None], axis=(1, 2))
    return dispatch, slot_weight


def expert_backward(expert_items):
    rows_in, grads_in, gate_w, up_w, down_w, scale_vec = expert_items
    gate_act = jnp.dot(rows_in, gate_w, preferred_element_type=jnp.float32)
    up_act = jnp.dot(rows_in, up_w, preferred_element_type=jnp.float32)
    sigmoid_gate = jax.nn.sigmoid(gate_act)
    silu_gate = gate_act * sigmoid_gate
    hidden_grad = jnp.dot(grads_in, down_w.T, preferred_element_type=jnp.float32)
    scale_grad = jnp.sum(hidden_grad * silu_gate * up_act, axis=0)
    scaled_grad = hidden_grad * scale_vec
    up_grad = (scaled_grad * silu_gate).astype(jnp.bfloat16)
    gate_grad = (scaled_grad * up_act * sigmoid_gate * (1.0 + gate_act * (1.0 - sigmoid_gate))).astype(jnp.bfloat16)
    input_rows = jnp.dot(gate_grad, gate_w.T, preferred_element_type=jnp.float32) + jnp.dot(up_grad, up_w.T, preferred_element_type=jnp.float32)
    return scale_grad, input_rows


def reference(tokens, cotangent, expert_ids, combine, w_gate, w_up, w_down, scale_vector):
    blocks = TOKENS // TOK_DEV
    dispatch, slot_weight = route_tables(expert_ids.reshape(blocks, TOK_DEV, 2), combine.reshape(blocks, TOK_DEV, 2), EXPERTS, CAP)
    token_blocks = tokens.astype(jnp.float32).reshape(blocks, TOK_DEV, D)
    cot_blocks = cotangent.astype(jnp.float32).reshape(blocks, TOK_DEV, D)
    sent_rows = jnp.einsum('bect,btd->becd', dispatch, token_blocks, precision=lax.Precision.HIGHEST).astype(jnp.bfloat16)
    cot_rows = jnp.einsum('bect,btd->becd', dispatch, cot_blocks, precision=lax.Precision.HIGHEST)
    sent_grads = (slot_weight[:, :, :, None] * cot_rows).astype(jnp.bfloat16)
    rows_by_expert = jnp.moveaxis(sent_rows, 1, 0).reshape(EXPERTS, blocks * CAP, D)
    grads_by_expert = jnp.moveaxis(sent_grads, 1, 0).reshape(EXPERTS, blocks * CAP, D)
    scale_grads, input_rows = lax.map(expert_backward, (rows_by_expert, grads_by_expert, w_gate, w_up, w_down, scale_vector))
    input_rows = jnp.moveaxis(input_rows.reshape(EXPERTS, blocks, CAP, D), 0, 1)
    token_grads = jnp.einsum('bect,becd->btd', dispatch, input_rows, precision=lax.Precision.HIGHEST)
    return token_grads.reshape(TOKENS, D).astype(jnp.bfloat16), scale_grads
```

```python
import functools

import jax
import jax.numpy as jnp
from jax import lax
from jax.experimental import pallas as pl
from jax.experimental.pallas import tpu as pltpu
from jax.sharding import PartitionSpec as P


def route_tables(expert_ids, combine, experts, capacity):
    blocks = expert_ids.shape[0]
    per_block = expert_ids.shape[1]
    onehot = (expert_ids[:, :, :, None] == jnp.arange(experts, dtype=jnp.int32)).astype(jnp.int32)
    flat_hits = onehot.reshape(blocks, per_block * 2, experts)
    earlier = jnp.cumsum(flat_hits, axis=1) - flat_hits
    slot_ids = jnp.sum(earlier * flat_hits, axis=2).reshape(blocks, per_block, 2)
    positions = (slot_ids[:, :, :, None] == jnp.arange(capacity, dtype=jnp.int32)).astype(
        jnp.float32
    )
    matches = onehot.astype(jnp.float32)[:, :, :, :, None] * positions[:, :, :, None, :]
    dispatch = jnp.transpose(jnp.sum(matches, axis=2), (0, 2, 3, 1))
    slot_weight = jnp.sum(matches * combine[:, :, :, None, None], axis=(1, 2))
    return (dispatch, slot_weight, slot_ids)


def combine_slots(slot_table, flat_index):
    tok_count = flat_index.shape[0]
    picked = jnp.take(slot_table, flat_index.reshape(-1), axis=0).reshape(
        tok_count, 2, slot_table.shape[1]
    )
    return picked[:, 0].astype(jnp.float32) + picked[:, 1].astype(jnp.float32)


MESH = pl.DeviceIdType.MESH
ROW_TILE = 16
SHORT_RING = 8
VMEM_LIMIT = 60 * 1024 * 1024


def ring_order(mesh):
    count = mesh.shape["dp"]
    devices = mesh.devices.reshape(count, -1)[:, 0]
    places = {}
    for index, device in enumerate(devices):
        coords = getattr(device, "coords", None)
        if coords is None:
            return tuple(range(count))
        places[(coords[2], coords[0])] = index
    zs = sorted({z for z, _ in places})
    xs = sorted({x for _, x in places})
    if len(places) != count or len(zs) * len(xs) != count or len(zs) % 2 or len(xs) < 2:
        return tuple(range(count))
    order = [places[(z, xs[0])] for z in zs]
    for turn, z in enumerate(reversed(zs)):
        order += [places[(z, x)] for x in (xs[1:] if turn % 2 == 0 else xs[:0:-1])]
    return tuple(order)


def lookup(table, key):
    found = jnp.int32(table[0])
    for index in range(1, len(table)):
        found = jnp.where(key == index, jnp.int32(table[index]), found)
    return found


def ring_place(ring):
    n = len(ring)
    position_of = [0] * n
    for position, index in enumerate(ring):
        position_of[index] = position
    position = lookup(position_of, lax.axis_index("dp"))
    right = lookup(ring, lax.rem(position + 1, n))
    left = lookup(ring, lax.rem(position + n - 1, n))
    return position, right, left


def greet(right, left):
    barrier = pltpu.get_barrier_semaphore()
    for neighbour in (left, right):
        pl.semaphore_signal(barrier, inc=1, device_id={"dp": neighbour}, device_id_type=MESH)
    pl.semaphore_wait(barrier, 2)


def gather_kernel(
    ring, tile, x_ref, gate_w, up_w, gate_ref, up_ref, grads_ref, rows_ref, w_buf, w_sem, own_sem,
    send_sem, recv_sem,
):
    n = len(ring)
    width = x_ref.shape[1] // 2
    rows = x_ref.shape[0]
    cut = rows // 2 // ROW_TILE * ROW_TILE
    tiles = gate_w.shape[1] // tile
    position, right, left = ring_place(ring)
    me = lax.axis_index("dp")
    halves = (pl.ds(0, cut), pl.ds(cut, rows - cut))

    def tile_columns(t):
        return pl.ds(0, tile) if tiles == 1 else pl.ds(pl.multiple_of(t * tile, tile), tile)

    def load(t, slot):
        columns = tile_columns(t)
        return (
            pltpu.make_async_copy(gate_w.at[:, columns], w_buf.at[slot, 0], w_sem.at[slot, 0]),
            pltpu.make_async_copy(up_w.at[:, columns], w_buf.at[slot, 1], w_sem.at[slot, 1]),
        )

    for copy in load(0, 0):
        copy.start()

    def columns_of(index):
        return pl.ds(pl.multiple_of(index * width, width), width)

    for which, full in enumerate((rows_ref, grads_ref)):
        own = pltpu.make_async_copy(
            x_ref.at[:, pl.ds(which * width, width)], full.at[:, columns_of(me)], own_sem.at[which]
        )
        own.start()
        own.wait()
    greet(right, left)

    def hop(which, step, way):
        full = (rows_ref, grads_ref)[which]
        shift = n - step if way == 0 else step
        origin = lookup(ring, lax.rem(position + shift, n))
        spot = full.at[halves[way], columns_of(origin)]
        return pltpu.make_async_remote_copy(
            src_ref=spot,
            dst_ref=spot,
            send_sem=send_sem.at[which, way, step],
            recv_sem=recv_sem.at[which, way, step],
            device_id={"dp": right if way == 0 else left},
            device_id_type=MESH,
        )

    def advance(which, step):
        for way in range(2):

            @pl.when(step > 0)
            def _():
                hop(which, step - 1, way).wait_recv()

            hop(which, step, way).start()

    def rows_step(step, carry):
        advance(0, step)
        return carry

    lax.fori_loop(0, n - 1, rows_step, 0)
    for way in range(2):
        hop(1, 0, way).start()
    for way in range(2):
        hop(0, n - 2, way).wait_recv()

    def grads_step(step, carry):
        @pl.when(step > 0)
        def _():
            advance(1, step)

        @pl.when(step < tiles)
        def _():
            slot = lax.rem(step, 2)

            @pl.when(step + 1 < tiles)
            def _():
                for copy in load(step + 1, lax.rem(step + 1, 2)):
                    copy.start()

            columns = tile_columns(step)
            for copy in load(step, slot):
                copy.wait()
            gate_ref[:, columns] = jnp.dot(
                rows_ref[...], w_buf[slot, 0], preferred_element_type=jnp.float32
            )
            up_ref[:, columns] = jnp.dot(
                rows_ref[...], w_buf[slot, 1], preferred_element_type=jnp.float32
            )

        return carry

    lax.fori_loop(0, n - 1, grads_step, 0)
    for way in range(2):
        hop(1, n - 2, way).wait_recv()

    def finish(step, carry):
        for which in range(2):
            for way in range(2):
                hop(which, step, way).wait_send()
        return carry

    lax.fori_loop(0, n - 1, finish, 0)


def gather_acts(ring, x, gate_w, up_w):
    n = len(ring)
    rows, width = x.shape[0], x.shape[1] // 2
    hidden = gate_w.shape[1]
    tile = 256 if hidden % 256 == 0 and hidden // 256 <= n - 1 else hidden
    full = n * width
    vmem = pl.BlockSpec(memory_space=pltpu.VMEM)
    anywhere = pl.BlockSpec(memory_space=pl.ANY)
    return pl.pallas_call(
        functools.partial(gather_kernel, ring, tile),
        out_shape=(
            jax.ShapeDtypeStruct((rows, hidden), jnp.float32),
            jax.ShapeDtypeStruct((rows, hidden), jnp.float32),
            jax.ShapeDtypeStruct((rows, full), jnp.bfloat16),
        ),
        in_specs=[anywhere, anywhere, anywhere],
        out_specs=(vmem, vmem, vmem),
        scratch_shapes=[
            pltpu.VMEM((rows, full), jnp.bfloat16),
            pltpu.VMEM((2, 2, full, tile), jnp.bfloat16),
            pltpu.SemaphoreType.DMA((2, 2)),
            pltpu.SemaphoreType.DMA((2,)),
            pltpu.SemaphoreType.DMA((2, 2, n - 1)),
            pltpu.SemaphoreType.DMA((2, 2, n - 1)),
        ],
        compiler_params=pltpu.CompilerParams(
            collective_id=0, has_side_effects=True, vmem_limit_bytes=VMEM_LIMIT
        ),
    )(x, gate_w, up_w)


def scatter_kernel(
    ring, gate_grad, up_grad, gate_w, up_w, out_ref, buf, w_buf, w_sem, send_sem, recv_sem
):
    n = len(ring)
    half = buf.shape[3]
    position, right, left = ring_place(ring)

    def load(step, slot):
        copies = []
        for way in range(2):
            shift = 2 * n - 1 - step if way == 0 else 1 + step
            owner = lookup(ring, lax.rem(position + shift, n))
            lines = pl.ds(pl.multiple_of(owner * (2 * half) + way * half, half), half)
            for kind, weight in enumerate((gate_w, up_w)):
                copies.append(
                    pltpu.make_async_copy(
                        weight.at[lines, :], w_buf.at[slot, way, kind], w_sem.at[slot, way, kind]
                    )
                )
        return copies

    for copy in load(0, 0):
        copy.start()
    greet(right, left)

    def hop(step, way):
        return pltpu.make_async_remote_copy(
            src_ref=buf.at[way, step],
            dst_ref=buf.at[way, step + 1],
            send_sem=send_sem.at[way, step],
            recv_sem=recv_sem.at[way, step],
            device_id={"dp": right if way == 0 else left},
            device_id_type=MESH,
        )

    def product(slot, way):
        across = (((1,), (1,)), ((), ()))
        return lax.dot_general(
            gate_grad[...], w_buf[slot, way, 0], across, preferred_element_type=jnp.float32
        ) + lax.dot_general(
            up_grad[...], w_buf[slot, way, 1], across, preferred_element_type=jnp.float32
        )

    def one_step(step, carry):
        slot = lax.rem(step, 2)

        @pl.when(step + 1 < n)
        def _():
            for copy in load(step + 1, lax.rem(step + 1, 2)):
                copy.start()

        for copy in load(step, slot):
            copy.wait()
        for way in range(2):
            part = product(slot, way)

            @pl.when(step == 0)
            def _():
                buf[way, 0] = part.astype(buf.dtype)

            @pl.when(step > 0)
            def _():
                hop(step - 1, way).wait_recv()
                total = buf[way, step].astype(jnp.float32) + part

                @pl.when(step < n - 1)
                def _():
                    buf[way, step] = total.astype(buf.dtype)

                @pl.when(step == n - 1)
                def _():
                    out_ref[way] = total.astype(out_ref.dtype)

            @pl.when(step < n - 1)
            def _():
                hop(step, way).start()

        return carry

    lax.fori_loop(0, n, one_step, 0)

    def finish(step, carry):
        for way in range(2):
            hop(step, way).wait_send()
        return carry

    lax.fori_loop(0, n - 1, finish, 0)


def scatter_rows(ring, gate_grad, up_grad, gate_w, up_w):
    n = len(ring)
    rows, hidden = gate_grad.shape
    half = gate_w.shape[0] // n // 2
    wire = jnp.bfloat16 if n <= SHORT_RING else jnp.float32
    vmem = pl.BlockSpec(memory_space=pltpu.VMEM)
    anywhere = pl.BlockSpec(memory_space=pl.ANY)
    return pl.pallas_call(
        functools.partial(scatter_kernel, ring),
        out_shape=jax.ShapeDtypeStruct((2, rows, half), wire),
        in_specs=[vmem, vmem, anywhere, anywhere],
        out_specs=vmem,
        scratch_shapes=[
            pltpu.VMEM((2, n, rows, half), wire),
            pltpu.VMEM((2, 2, 2, half, hidden), jnp.bfloat16),
            pltpu.SemaphoreType.DMA((2, 2, 2)),
            pltpu.SemaphoreType.DMA((2, n - 1)),
            pltpu.SemaphoreType.DMA((2, n - 1)),
        ],
        compiler_params=pltpu.CompilerParams(
            collective_id=1, has_side_effects=True, vmem_limit_bytes=VMEM_LIMIT
        ),
    )(gate_grad, up_grad, gate_w, up_w)


def local(ring, tokens, cotangent, expert_ids, combine, w_gate, w_up, w_down, scale_vector):
    experts = lax.axis_size("expert")
    tok_count = tokens.shape[0]
    capacity = 2 * tok_count // experts + 1
    dispatch, slot_weight, slot_ids = route_tables(
        expert_ids[None], combine[None], experts, capacity
    )
    dispatch_half = dispatch[0].astype(jnp.bfloat16)
    slot_weight = slot_weight[0]
    flat_index = expert_ids * capacity + slot_ids[0]
    sent_rows = jnp.einsum(
        "ect,td->ecd", dispatch_half, tokens, preferred_element_type=jnp.float32
    ).astype(jnp.bfloat16)
    cot_rows = jnp.einsum(
        "ect,td->ecd", dispatch_half, cotangent, preferred_element_type=jnp.float32
    )
    sent_grads = (slot_weight[:, :, None] * cot_rows).astype(jnp.bfloat16)
    sent = jnp.concatenate([sent_rows, sent_grads], axis=2)
    got = lax.all_to_all(sent, "expert", split_axis=0, concat_axis=0, tiled=True)
    row_count = experts * capacity
    padding = -row_count % ROW_TILE
    x = jnp.pad(got.reshape(row_count, got.shape[2]), ((0, padding), (0, 0)))
    gate_w = w_gate[0]
    up_w = w_up[0]
    down_w = w_down[0]
    gate_act, up_act, grads = gather_acts(ring, x, gate_w, up_w)
    hidden_grad = lax.dot_general(
        grads, down_w, (((1,), (1,)), ((), ())), preferred_element_type=jnp.float32
    )
    sigmoid_gate = jax.nn.sigmoid(gate_act)
    silu_gate = gate_act * sigmoid_gate
    scale_grad = jnp.sum(hidden_grad * silu_gate * up_act, axis=0)
    scaled_grad = hidden_grad * scale_vector[0]
    up_grad = (scaled_grad * silu_gate).astype(jnp.bfloat16)
    gate_grad = (
        scaled_grad * up_act * sigmoid_gate * (1.0 + gate_act * (1.0 - sigmoid_gate))
    ).astype(jnp.bfloat16)
    halves = scatter_rows(ring, gate_grad, up_grad, gate_w, up_w)
    summed = jnp.concatenate([halves[0], halves[1]], axis=1)[:row_count]
    slot_part = summed.reshape(experts, capacity, summed.shape[1])
    returned = lax.all_to_all(slot_part, "expert", split_axis=0, concat_axis=0, tiled=True)
    token_grads = combine_slots(returned.reshape(row_count, returned.shape[2]), flat_index)
    return (token_grads.astype(jnp.bfloat16), scale_grad[None, :])


def solution(mesh):
    placed = (
        P("expert", "dp"),
        P("expert", "dp"),
        P("expert", None),
        P("expert", None),
        P("expert", None, "dp"),
        P("expert", None, "dp"),
        P("expert", "dp", None),
        P("expert", "dp"),
    )
    return jax.shard_map(
        functools.partial(local, ring_order(mesh)),
        mesh=mesh,
        in_specs=placed,
        out_specs=(P("expert", "dp"), P("expert", "dp")),
        check_vma=False,
    )
```
